256 devices in a mesh: grp: 2 (over y), slab: 32 (over z, core), ang: 4 (over x).
Axes of the slice: x: 4, y: 2, z: 16, core: 2. Of those that a mesh axis runs over, the one named last changes fastest.
The devices are a block of a 4x16x16 slice.
Arguments:
- volume: bfloat16 [128, 256, 1024], P(('grp', 'slab')), parts along dimension 0, may hold values from -6 to 6
- ray_weights: bfloat16 [8, 1024, 1024], P('ang'), may hold values from -0.0234375 to 0.0234375
- row_offsets: int32 [8, 64], P('ang'), may hold values from 0 to 8
- measured: float32 [16, 256, 1024], P(('grp', 'ang'), 'slab'), parts along dimension 0, may hold values from -6 to 6
- shifts: float32 [16], P(('grp', 'ang')), parts along dimension 0, may hold values from -4 to 4
Outputs:
- updated_volume: bfloat16 [128, 256, 1024], P(('grp', 'slab')), parts along dimension 0
- last_residual: float32 [16, 256, 1024], P(('grp', 'ang'), 'slab'), parts along dimension 0
- shift_slope: float32 [16], P(('grp', 'ang')), parts along dimension 0
The draws below stay inside these ranges and needn't reach their ends.
There are 2 independent parts, one for each index of `grp`. The reference program is written for one: setup_inputs(seed, part) draws one part's arguments, and reference() takes and returns one part's arrays. A program takes and returns all parts, laid end to end along the dimension named above; an argument that names none is the same for every part. Nothing has to cross between parts.
All inputs are finite; a program needn't handle non-finite values.
Results may differ from the reference program's by a relative error of at most 0.006.
Values may be sent and summed in bfloat16 or wider, within the bound.
No kernel may reach another device: no remote copies, remote signals or barrier semaphores. Data moves between devices by JAX's collectives and lax.ppermute only.
A program may use at most 128 MiB of HBM per device.

```python
import math
import jax
import jax.numpy as jnp
from jax import lax

ANG_DEV = 2
Y = 256
X = 1024
U = 1024
OFF = 8
ROUNDS = 2
NZ = 64
ANGLES = 8
N_ANG = 4


def touch_ends(entries, stream_key, least, high):
    extent = entries.shape
    index_at = [jax.random.randint(jax.random.fold_in(stream_key, axis), (), 0, extent[axis]) for axis in range(len(extent))]
    entries = entries.at[tuple(index_at)].set(least)
    longest = extent.index(max(extent))
    index_at[longest] = (index_at[longest] + 1) % extent[longest]
    return entries.at[tuple(index_at)].set(high)


def level_of(key, dims, split, smallest, largest):
    factor_of = 1.0
    for axis_at, parts in split:
        draws = jax.random.uniform(jax.random.fold_in(jax.random.fold_in(key, 6), axis_at), (parts,), jnp.float32, smallest / len(split), largest / len(split))
        factor_of = factor_of * jnp.repeat(jnp.exp(draws), dims[axis_at] // parts).reshape((-1,) + (1,) * (len(dims) - 1 - axis_at))
    return factor_of


def scatter_about(stream_key, dims, scale, limit, shards=(), dtype=jnp.bfloat16):
    result = scale * jax.random.normal(stream_key, dims, jnp.float32)
    if shards:
        result = result * level_of(stream_key, dims, shards, -0.22, 0.18)
    return jnp.clip(result, -limit, limit).astype(dtype)


def setup_inputs(seed: int = 0, part: int = 0) -> dict:
    splits = jax.random.split(jax.random.key(seed), 6)
    part_splits = jax.random.split(jax.random.fold_in(splits[5], part), 6)
    volume = scatter_about(part_splits[0], (NZ, Y, X), 1.0, 6.0, ((0, 32),))
    ray_weights = scatter_about(splits[1], (ANGLES, X, U), (X * NZ) ** -0.5, 0.0234375, ((0, 4),))
    row_offsets = touch_ends(jax.random.randint(splits[2], (ANGLES, NZ), 0, OFF + 1), jax.random.fold_in(splits[2], 1), 0, OFF).astype(jnp.int32)
    measured = scatter_about(part_splits[3], (ANGLES, Y, U), 1.0, 6.0, ((0, 4), (1, 32)), jnp.float32)
    shifts = jnp.clip(jax.random.uniform(part_splits[4], (ANGLES,), jnp.float32, -4.0, 4.0) * level_of(part_splits[4], (ANGLES,), ((0, 4),), -0.4, 0.0), -4.0, 4.0)
    return dict(volume=volume, ray_weights=ray_weights, row_offsets=row_offsets, measured=measured, shifts=shifts)


step_size = 0.5

def move_down(products, tilt_table):
    base = jnp.zeros((Y + OFF, U), jnp.float32)
    placed = jax.vmap(lambda block, shift_rows: lax.dynamic_update_slice(base, block, (shift_rows, jnp.int32(0))))(products, tilt_table)
    return lax.optimization_barrier(jnp.sum(placed, axis=0))[:Y]

def reference(volume, ray_weights, row_offsets, measured, shifts):
    frequency = jnp.fft.fftfreq(U).astype(jnp.float32)
    spectrum = jnp.fft.fft(measured.astype(jnp.float32), axis=-1)
    phase = jnp.exp(-2j * jnp.pi * frequency[None, :] * shifts[:, None])
    rotated = spectrum * phase[:, None, :]
    shifted = jnp.real(jnp.fft.ifft(rotated, axis=-1)).astype(jnp.float32)
    slope_field = jnp.real(jnp.fft.ifft(rotated * (-2j * jnp.pi * frequency)[None, None, :], axis=-1)).astype(jnp.float32)
    current = volume
    projection = shifted
    residual = shifted
    for round_index in range(ROUNDS):
        flattened = current.astype(jnp.float32).reshape(NZ * Y, X)
        projection = jnp.stack([move_down(jnp.dot(flattened, ray_weights[angle_index].astype(jnp.float32), preferred_element_type=jnp.float32).reshape(NZ, Y, U), row_offsets[angle_index]) for angle_index in range(ANGLES)])
        residual = projection - shifted
        rounded = residual.astype(jnp.bfloat16)
        padded = jnp.concatenate([rounded, jnp.zeros((ANGLES, OFF, U), jnp.bfloat16)], axis=1)
        gradient = jnp.zeros((NZ * Y, X), jnp.float32)
        for group_index in range(N_ANG):
            running = jnp.zeros((NZ * Y, X), jnp.float32)
            for angle_index in range(group_index * ANG_DEV, (group_index + 1) * ANG_DEV):
                source = padded[angle_index]
                picked = jax.vmap(lambda shift_rows: lax.dynamic_slice(source, (shift_rows, jnp.int32(0)), (Y, U)))(row_offsets[angle_index])
                running = running + jnp.dot(picked.reshape(NZ * Y, U).astype(jnp.float32), ray_weights[angle_index].astype(jnp.float32).T, preferred_element_type=jnp.float32)
            partial_value = lax.optimization_barrier(running.astype(jnp.bfloat16))
            gradient = gradient + partial_value.astype(jnp.float32)
        current = (current.astype(jnp.float32) - step_size * gradient.reshape(NZ, Y, X)).astype(jnp.bfloat16)
    shift_slope = lax.optimization_barrier(jnp.sum(projection * slope_field, axis=(1, 2))) / math.sqrt(Y * U)
    return (current, residual, shift_slope)
```

```python
import math

import jax
import jax.numpy as jnp
from jax import lax
from jax.sharding import PartitionSpec as P

OFF = 8
ROUNDS = 2
STEP_SIZE = 0.5


def moments(length):
    waves = [2.0 * math.pi * k / length for k in range(-(length // 2), length // 2)]
    return [sum(w**p for w in waves) / length for p in (2, 4, 6, 8)]


def interpolation_kernels(shifts, taps, length):
    whole = jnp.round(shifts)
    part = shifts - whole
    odd_shift = 1.0 - 2.0 * (whole.astype(jnp.int32) & 1).astype(jnp.float32)
    sine = odd_shift * jnp.sin(math.pi * part)
    cosine = odd_shift * jnp.cos(math.pi * part)
    v = lax.broadcasted_iota(jnp.int32, (1, taps, length), 1)
    u = lax.broadcasted_iota(jnp.int32, (1, taps, length), 2)
    lag = u - v
    lag = jnp.where(lag >= length // 2, lag - length, jnp.where(lag < -(length // 2), lag + length, lag))
    sign = 1.0 - 2.0 * (lag & 1).astype(jnp.float32)
    d = (lag - whole.astype(jnp.int32)[:, None, None]).astype(jnp.float32) - part[:, None, None]
    near = jnp.abs(d) < 0.1
    safe = jnp.where(near, 1.0, d)
    y = safe * (math.pi / length)
    sin_y = jnp.sin(y)
    cos_y = jnp.cos(y)
    inv = 1.0 / sin_y
    cot = cos_y * inv
    sin_d = -sign * sine[:, None, None]
    cos_d = sign * cosine[:, None, None]
    far_h = sin_d * cot * (1.0 / length)
    far_q = (math.pi / length) * (sin_d * inv * inv * (1.0 / length) - cos_d * cot)
    m2, m4, m6, m8 = moments(length)
    s = d * d
    near_h = 1.0 - s * (m2 / 2 - s * (m4 / 24 - s * (m6 / 720 - s * (m8 / 40320))))
    near_q = d * (m2 - s * (m4 / 6 - s * (m6 / 120 - s * (m8 / 5040))))
    return jnp.where(near, near_h, far_h), jnp.where(near, near_q, far_q)


def registered(measured, shifts):
    angles, rows, length = measured.shape
    taps = 128
    blocks = length // taps
    h, q = interpolation_kernels(shifts, taps, length)
    kernels = jnp.concatenate([h, q], axis=2)
    pieces = measured.reshape(angles, rows, blocks, taps).transpose(0, 2, 1, 3)
    pieces = pieces.reshape(angles, blocks * rows, taps)
    spread = jnp.einsum("avr,aru->avu", pieces, kernels, precision=lax.Precision.HIGHEST)
    spread = spread.reshape(angles, blocks, rows, 2, length)
    total = spread[:, 0]
    for k in range(1, blocks):
        total = total + jnp.roll(spread[:, k], taps * k, axis=-1)
    return total[:, :, 0], total[:, :, 1]


def make_per_device(slab):
    def per_device(volume, ray_weights, row_offsets, measured, shifts):
        slices_here, rows_all, cells = volume.shape
        angles_here, band, columns = measured.shape
        slabs = lax.axis_size(slab)
        angs = lax.axis_size("ang")
        chunk = cells // angs
        slices = slices_here * slabs
        angles = angles_here * angs
        f32 = jnp.float32
        bf16 = jnp.bfloat16

        mine = lax.dynamic_slice_in_dim(volume, lax.axis_index("ang") * chunk, chunk, 2)
        mine = mine.reshape(slices_here, slabs, band, chunk).transpose(1, 0, 2, 3)
        own = lax.all_to_all(mine, slab, 0, 0, tiled=True).reshape(slices, band, chunk)
        down_ring = [(i, i + 1) for i in range(slabs - 1)]
        up_ring = [(i + 1, i) for i in range(slabs - 1)]
        above = lax.ppermute(own, slab, down_ring)
        current = jnp.concatenate([above, own], axis=1)

        copies = jnp.broadcast_to(row_offsets, (angs, *row_offsets.shape))
        table = lax.all_to_all(copies, "ang", 0, 0, tiled=True).reshape(angles, slices)

        shifted, slope_field = registered(measured, shifts)

        shape = (angles, band, slices, 2 * band)
        y = lax.broadcasted_iota(jnp.int32, shape, 1)
        r = lax.broadcasted_iota(jnp.int32, shape, 3)
        held = (r >= band) | (lax.axis_index(slab) > 0)
        gather = (r - band == y - table[:, None, :, None]) & held
        gather = gather.astype(bf16).reshape(angles * band, slices * 2 * band)
        shape = (slices, 2 * band, angles, 3 * band)
        r = lax.broadcasted_iota(jnp.int32, shape, 1)
        t = lax.broadcasted_iota(jnp.int32, shape, 3)
        scatter = (t == r + table.T[:, None, :, None]).astype(bf16)

        for round_index in range(ROUNDS):
            last = round_index == ROUNDS - 1
            stacked = jnp.dot(
                gather, current.reshape(slices * 2 * band, chunk), preferred_element_type=f32
            )
            high = lax.reduce_precision(stacked, 8, 7)
            parts = jnp.stack([high.astype(bf16), (stacked - high).astype(bf16)])
            parts = parts.reshape(2, angs, angles_here, band, chunk).transpose(1, 2, 0, 3, 4)
            parts = lax.all_to_all(parts, "ang", 0, 0, tiled=True)
            parts = parts.transpose(1, 2, 3, 0, 4).reshape(angles_here, 2 * band, cells)
            product = jnp.einsum("arx,axu->aru", parts, ray_weights, preferred_element_type=f32)
            projection = product[:, :band] + product[:, band:]
            residual = projection - shifted
            rounded = residual.astype(bf16)
            back = jnp.einsum("aru,axu->arx", rounded, ray_weights, preferred_element_type=f32)
            back = back.astype(bf16).reshape(angles_here, band, angs, chunk).transpose(2, 0, 1, 3)
            back = lax.all_to_all(back, "ang", 0, 0, tiled=True).reshape(angles, band, chunk)
            below = lax.ppermute(back, slab, up_ring)
            if last:
                window = jnp.concatenate([back, below], axis=1)
                pick = scatter[:, band:, :, band:].reshape(slices * band, angles * 2 * band)
                before = current[:, band:]
            else:
                window = jnp.concatenate([lax.ppermute(back, slab, down_ring), back, below], axis=1)
                pick = scatter.reshape(slices * 2 * band, angles * 3 * band)
                before = current
            gradient = jnp.dot(pick, window.reshape(-1, chunk), preferred_element_type=f32)
            current = (before.astype(f32) - STEP_SIZE * gradient.reshape(before.shape)).astype(bf16)

        local_dot = jnp.sum(projection * slope_field, axis=(1, 2))
        dots = jnp.broadcast_to(local_dot, (slabs, angles_here))
        dots = lax.all_to_all(dots, slab, 0, 0, tiled=True)
        shift_slope = jnp.sum(dots, axis=0) / math.sqrt(rows_all * columns)

        home = current.reshape(slabs, slices_here, band, chunk)
        home = lax.all_to_all(home, slab, 0, 0, tiled=True).transpose(1, 0, 2, 3)
        home = home.reshape(slices_here, rows_all, chunk)
        spread = jnp.broadcast_to(home, (angs, *home.shape))
        spread = lax.all_to_all(spread, "ang", 0, 0, tiled=True)
        updated = spread.transpose(1, 2, 0, 3).reshape(slices_here, rows_all, cells)
        return updated, residual, shift_slope

    return per_device


def solution(mesh):
    return jax.shard_map(
        make_per_device("slab"),
        mesh=mesh,
        in_specs=(
            P(("grp", "slab"), None, None),
            P("ang", None, None),
            P("ang", None),
            P(("grp", "ang"), "slab", None),
            P(("grp", "ang")),
        ),
        out_specs=(P(("grp", "slab"), None, None), P(("grp", "ang"), "slab", None), P(("grp", "ang"))),
        check_vma=False,
    )
```

```python
import math

import jax
import jax.numpy as jnp
from jax import lax
from jax.experimental import pallas as pl
from jax.experimental.pallas import tpu as pltpu
from jax.sharding import Mesh
from jax.sharding import PartitionSpec as P

OFF = 8
ROUNDS = 2
STEP_SIZE = 0.5


def moments(length):
    waves = [2.0 * math.pi * k / length for k in range(-(length // 2), length // 2)]
    return [sum(w**p for w in waves) / length for p in (2, 4, 6, 8)]


def interpolation_kernels(shifts, taps, length):
    whole = jnp.round(shifts)
    part = shifts - whole
    odd_shift = 1.0 - 2.0 * (whole.astype(jnp.int32) & 1).astype(jnp.float32)
    sine = odd_shift * jnp.sin(math.pi * part)
    cosine = odd_shift * jnp.cos(math.pi * part)
    v = lax.broadcasted_iota(jnp.int32, (1, taps, length), 1)
    u = lax.broadcasted_iota(jnp.int32, (1, taps, length), 2)
    lag = u - v
    lag = jnp.where(lag >= length // 2, lag - length, jnp.where(lag < -(length // 2), lag + length, lag))
    sign = 1.0 - 2.0 * (lag & 1).astype(jnp.float32)
    d = (lag - whole.astype(jnp.int32)[:, None, None]).astype(jnp.float32) - part[:, None, None]
    near = jnp.abs(d) < 0.1
    safe = jnp.where(near, 1.0, d)
    y = safe * (math.pi / length)
    sin_y = jnp.sin(y)
    cos_y = jnp.cos(y)
    inv = 1.0 / sin_y
    cot = cos_y * inv
    sin_d = -sign * sine[:, None, None]
    cos_d = sign * cosine[:, None, None]
    far_h = sin_d * cot * (1.0 / length)
    far_q = (math.pi / length) * (sin_d * inv * inv * (1.0 / length) - cos_d * cot)
    m2, m4, m6, m8 = moments(length)
    s = d * d
    near_h = 1.0 - s * (m2 / 2 - s * (m4 / 24 - s * (m6 / 720 - s * (m8 / 40320))))
    near_q = d * (m2 - s * (m4 / 6 - s * (m6 / 120 - s * (m8 / 5040))))
    return jnp.where(near, near_h, far_h), jnp.where(near, near_q, far_q)


def registered(measured, shifts):
    angles, rows, length = measured.shape
    taps = 128
    blocks = length // taps
    h, q = interpolation_kernels(shifts, taps, length)
    kernels = jnp.concatenate([h, q], axis=2)
    pieces = measured.reshape(angles, rows, blocks, taps).transpose(0, 2, 1, 3)
    pieces = pieces.reshape(angles, blocks * rows, taps)
    spread = jnp.einsum("avr,aru->avu", pieces, kernels, precision=lax.Precision.HIGHEST)
    spread = spread.reshape(angles, blocks, rows, 2, length)
    total = spread[:, 0]
    for k in range(1, blocks):
        total = total + jnp.roll(spread[:, k], taps * k, axis=-1)
    return total[:, :, 0], total[:, :, 1]


SLAB = ("z", "core")


def from_ang(blocks, step):
    size = len(blocks)
    return [
        blocks[k] if k == 0 else lax.ppermute(blocks[k], "ang", [(i, (i + k * step) % size) for i in range(size)])
        for k in range(size)
    ]


def swap_cores(pair):
    first = lax.axis_index("core") == 0
    kept = jnp.where(first, pair[0], pair[1])
    sent = jnp.where(first, pair[1], pair[0])
    got = lax.ppermute(sent, "core", [(0, 1), (1, 0)])
    return jnp.where(first, kept, got), jnp.where(first, got, kept)


def place_chunks(chunks):
    count = len(chunks)
    slices, rows, width = chunks[0].shape

    def kernel(*refs):
        sources, out, sems = refs[:count], refs[count], refs[count + 1]
        here = lax.axis_index("ang")
        copies = []
        for k in range(count):
            start = pl.multiple_of(lax.rem(here + k, count) * width, width)
            copies.append(pltpu.make_async_copy(sources[k], out.at[:, :, pl.ds(start, width)], sems.at[k]))
            copies[-1].start()
        for copy in copies:
            copy.wait()

    return pl.pallas_call(
        kernel,
        out_shape=jax.ShapeDtypeStruct((slices, rows, width * count), chunks[0].dtype),
        in_specs=[pl.BlockSpec(memory_space=pl.ANY)] * count,
        out_specs=pl.BlockSpec(memory_space=pl.ANY),
        scratch_shapes=[pltpu.SemaphoreType.DMA((count,))],
    )(*chunks)


def per_device(volume, ray_weights, row_offsets, measured, shifts):
    slices_here, rows_all, cells = volume.shape
    angles_here, band, columns = measured.shape
    chips = lax.axis_size("z")
    slabs = lax.axis_size(SLAB)
    angs = lax.axis_size("ang")
    here = lax.axis_index("ang")
    chunk = cells // angs
    slices = slices_here * slabs
    angles = angles_here * angs
    f32 = jnp.float32
    bf16 = jnp.bfloat16
    down_ring = [(i, i + 1) for i in range(slabs - 1)]
    up_ring = [(i + 1, i) for i in range(slabs - 1)]

    table = jnp.stack(from_ang([row_offsets] * angs, -1)).reshape(angles, slices)

    mine = lax.dynamic_slice_in_dim(volume, here * chunk, chunk, 2)
    mine = mine.reshape(slices_here, chips, 2, band, chunk).transpose(2, 1, 0, 3, 4)
    mine = jnp.stack(swap_cores(mine), axis=1)
    own = lax.all_to_all(mine, "z", 0, 0, tiled=True).reshape(slices, band, chunk)
    above = lax.ppermute(own, SLAB, down_ring)
    current = jnp.concatenate([above, own], axis=1)

    weights = ray_weights.reshape(angles_here, angs, chunk, columns)
    weights = jnp.concatenate(
        [lax.dynamic_slice_in_dim(weights, (here + angs - k) % angs, 1, 1) for k in range(angs)], axis=1
    ).reshape(angles_here, cells, columns)

    shifted, slope_field = registered(measured, shifts)

    shape = (angles, band, slices, 2 * band)
    y = lax.broadcasted_iota(jnp.int32, shape, 1)
    r = lax.broadcasted_iota(jnp.int32, shape, 3)
    held = (r >= band) | (lax.axis_index(SLAB) > 0)
    gather = (r - band == y - table[:, None, :, None]) & held
    gather = gather.astype(bf16).reshape(angles * band, slices * 2 * band)
    shape = (slices, 2 * band, angles, 3 * band)
    r = lax.broadcasted_iota(jnp.int32, shape, 1)
    t = lax.broadcasted_iota(jnp.int32, shape, 3)
    scatter = (t == r + table.T[:, None, :, None]).astype(bf16)

    for round_index in range(ROUNDS):
        last = round_index == ROUNDS - 1
        stacked = jnp.dot(gather, current.reshape(slices * 2 * band, chunk), preferred_element_type=f32)
        high = lax.reduce_precision(stacked, 8, 7)
        high, low = (
            x.astype(bf16).reshape(angs, angles_here, band, chunk) for x in (high, stacked - high)
        )
        parts = from_ang([jnp.concatenate([high[k], low[k]], axis=1) for k in range(angs)], 1)
        parts = jnp.concatenate(parts, axis=2)
        product = jnp.einsum("arx,axu->aru", parts, weights, preferred_element_type=f32)
        projection = product[:, :band] + product[:, band:]
        residual = projection - shifted
        rounded = residual.astype(bf16)
        back = jnp.einsum("aru,axu->arx", rounded, weights, preferred_element_type=f32).astype(bf16)
        back = from_ang([back[:, :, k * chunk : (k + 1) * chunk] for k in range(angs)], -1)
        back = jnp.concatenate(back, axis=0)
        below = lax.ppermute(back, SLAB, up_ring)
        if last:
            window = jnp.concatenate([back, below], axis=1)
            pick = scatter[:, band:, :, band:].reshape(slices * band, angles * 2 * band)
            before = current[:, band:]
        else:
            window = jnp.concatenate([lax.ppermute(back, SLAB, down_ring), back, below], axis=1)
            pick = scatter.reshape(slices * 2 * band, angles * 3 * band)
            before = current
        gradient = jnp.dot(pick, window.reshape(-1, chunk), preferred_element_type=f32)
        current = (before.astype(f32) - STEP_SIZE * gradient.reshape(before.shape)).astype(bf16)

    home = current.reshape(chips, 2, slices_here, band, chunk)
    dots = jnp.sum(projection * slope_field, axis=(1, 2))
    dots, home = lax.optimization_barrier((dots, home))
    home = lax.all_to_all(home, "z", 0, 0, tiled=True)
    bit = 1
    while bit < slabs:
        dots = dots + lax.ppermute(dots, SLAB, [(i, i ^ bit) for i in range(slabs)])
        bit *= 2
    shift_slope = dots / math.sqrt(rows_all * columns)
    home = jnp.stack(swap_cores(home.transpose(1, 2, 0, 3, 4)), axis=2)
    home = home.reshape(slices_here, rows_all, chunk)
    ahead = [(i, (i + 1) % angs) for i in range(angs)]
    behind = [((i + 1) % angs, i) for i in range(angs)]
    half = slices_here // 2
    lower = lax.ppermute(home, "ang", ahead)
    upper = lax.ppermute(home, "ang", behind)
    far = [lax.ppermute(lower[:half], "ang", ahead), lax.ppermute(upper[half:], "ang", behind)]
    updated = place_chunks([home, upper, jnp.concatenate(far), lower])
    return updated, residual, shift_slope


def solution(mesh):
    slabs = mesh.shape["slab"]
    split = Mesh(
        mesh.devices.reshape(mesh.shape["grp"], slabs // 2, 2, mesh.shape["ang"]),
        ("grp", "z", "core", "ang"),
    )
    part = ("grp", "z", "core")
    return jax.shard_map(
        per_device,
        mesh=split,
        in_specs=(P(part, None, None), P("ang", None, None), P("ang", None), P(("grp", "ang"), SLAB, None), P(("grp", "ang"))),
        out_specs=(P(part, None, None), P(("grp", "ang"), SLAB, None), P(("grp", "ang"))),
        check_vma=False,
    )
```

```python
import math

import jax
import jax.numpy as jnp
from jax import lax
from jax.sharding import PartitionSpec as P

OFF = 8
ROUNDS = 2
STEP_SIZE = 0.5


def moments(length):
    waves = [2.0 * math.pi * k / length for k in range(-(length // 2), length // 2)]
    return [sum(w**p for w in waves) / length for p in (2, 4, 6, 8)]


def interpolation_kernels(shifts, taps, length):
    whole = jnp.round(shifts)
    part = shifts - whole
    odd_shift = 1.0 - 2.0 * (whole.astype(jnp.int32) & 1).astype(jnp.float32)
    sine = odd_shift * jnp.sin(math.pi * part)
    cosine = odd_shift * jnp.cos(math.pi * part)
    v = lax.broadcasted_iota(jnp.int32, (1, taps, length), 1)
    u = lax.broadcasted_iota(jnp.int32, (1, taps, length), 2)
    lag = u - v
    lag = jnp.where(lag >= length // 2, lag - length, jnp.where(lag < -(length // 2), lag + length, lag))
    sign = 1.0 - 2.0 * (lag & 1).astype(jnp.float32)
    d = (lag - whole.astype(jnp.int32)[:, None, None]).astype(jnp.float32) - part[:, None, None]
    near = jnp.abs(d) < 0.1
    safe = jnp.where(near, 1.0, d)
    y = safe * (math.pi / length)
    sin_y = jnp.sin(y)
    cos_y = jnp.cos(y)
    inv = 1.0 / sin_y
    cot = cos_y * inv
    sin_d = -sign * sine[:, None, None]
    cos_d = sign * cosine[:, None, None]
    far_h = sin_d * cot * (1.0 / length)
    far_q = (math.pi / length) * (sin_d * inv * inv * (1.0 / length) - cos_d * cot)
    m2, m4, m6, m8 = moments(length)
    s = d * d
    near_h = 1.0 - s * (m2 / 2 - s * (m4 / 24 - s * (m6 / 720 - s * (m8 / 40320))))
    near_q = d * (m2 - s * (m4 / 6 - s * (m6 / 120 - s * (m8 / 5040))))
    return jnp.where(near, near_h, far_h), jnp.where(near, near_q, far_q)


def registered(measured, shifts):
    angles, rows, length = measured.shape
    taps = 128
    blocks = length // taps
    h, q = interpolation_kernels(shifts, taps, length)
    kernels = jnp.concatenate([h, q], axis=2)
    pieces = measured.reshape(angles, rows, blocks, taps).transpose(0, 2, 1, 3)
    pieces = pieces.reshape(angles, blocks * rows, taps)
    spread = jnp.einsum("avr,aru->avu", pieces, kernels, precision=lax.Precision.HIGHEST)
    spread = spread.reshape(angles, blocks, rows, 2, length)
    total = spread[:, 0]
    for k in range(1, blocks):
        total = total + jnp.roll(spread[:, k], taps * k, axis=-1)
    return total[:, :, 0], total[:, :, 1]


SLAB = "slab"


def from_ang(blocks, step):
    size = len(blocks)
    return [
        blocks[k] if k == 0 else lax.ppermute(blocks[k], "ang", [(i, (i + k * step) % size) for i in range(size)])
        for k in range(size)
    ]


def split_parts(value, count):
    parts = []
    for _ in range(count):
        high = lax.reduce_precision(value, 8, 7)
        parts.append(high.astype(jnp.bfloat16))
        value = value - high
    return parts


def in_order(chunks):
    count = len(chunks)
    here = lax.axis_index("ang")

    def pick(column):
        found = chunks[column]
        for k in range(1, count):
            found = jnp.where(here == k, chunks[(column - k) % count], found)
        return found

    return jnp.concatenate([pick(column) for column in range(count)], axis=2)


def per_device(volume, ray_weights, row_offsets, measured, shifts):
    slices_here, rows_all, cells = volume.shape
    angles_here, band, columns = measured.shape
    slabs = lax.axis_size(SLAB)
    angs = lax.axis_size("ang")
    here = lax.axis_index("ang")
    chunk = cells // angs
    slices = slices_here * slabs
    angles = angles_here * angs
    f32 = jnp.float32
    bf16 = jnp.bfloat16
    down_ring = [(i, i + 1) for i in range(slabs - 1)]
    up_ring = [(i + 1, i) for i in range(slabs - 1)]

    table = jnp.stack(from_ang([row_offsets] * angs, -1)).reshape(angles, slices)

    mine = lax.dynamic_slice_in_dim(volume, here * chunk, chunk, 2)
    mine = mine.reshape(slices_here, slabs, band, chunk).transpose(1, 0, 2, 3)
    own = lax.all_to_all(mine, SLAB, 0, 0, tiled=True).reshape(slices, band, chunk)
    above = lax.ppermute(own, SLAB, down_ring)
    current = jnp.concatenate([above, own], axis=1)

    weights = ray_weights.reshape(angles_here, angs, chunk, columns)
    weights = jnp.concatenate(
        [lax.dynamic_slice_in_dim(weights, (here + angs - k) % angs, 1, 1) for k in range(angs)], axis=1
    ).reshape(angles_here, cells, columns)

    shifted, slope_field = registered(measured, shifts)

    places = slices * 2 * band
    spread = lax.broadcasted_iota(jnp.int32, (slices, places), 0) == lax.broadcasted_iota(
        jnp.int32, (slices, places), 1
    ) // (2 * band)
    offsets = jnp.dot(table.astype(bf16), spread.astype(bf16), preferred_element_type=f32)
    shape = (angles, band, places)
    y = lax.broadcasted_iota(jnp.int32, shape, 1)
    r = lax.broadcasted_iota(jnp.int32, shape, 2) % (2 * band)
    held = (r >= band) | (lax.axis_index(SLAB) > 0)
    gather = (y - (r - band) == offsets.astype(jnp.int32)[:, None, :]) & held
    gather = gather.astype(bf16).reshape(angles * band, places)
    shape = (slices, 2 * band, angles, 3 * band)
    r = lax.broadcasted_iota(jnp.int32, shape, 1)
    t = lax.broadcasted_iota(jnp.int32, shape, 3)
    scatter = (t == r + table.T[:, None, :, None]).astype(bf16)

    for round_index in range(ROUNDS):
        last = round_index == ROUNDS - 1
        stacked = jnp.dot(gather, current.reshape(slices * 2 * band, chunk), preferred_element_type=f32)
        high, low = (
            x.reshape(angs, angles_here, band, chunk) for x in split_parts(stacked, 2)
        )
        parts = from_ang([jnp.concatenate([high[k], low[k]], axis=1) for k in range(angs)], 1)
        parts = jnp.concatenate(parts, axis=2)
        product = jnp.einsum("arx,axu->aru", parts, weights, preferred_element_type=f32)
        projection = product[:, :band] + product[:, band:]
        residual = projection - shifted
        rounded = residual.astype(bf16)
        back = jnp.einsum("aru,axu->arx", rounded, weights, preferred_element_type=f32).astype(bf16)
        back = from_ang([back[:, :, k * chunk : (k + 1) * chunk] for k in range(angs)], -1)
        back = jnp.concatenate(back, axis=0)
        below = lax.ppermute(back, SLAB, up_ring)
        if last:
            window = jnp.concatenate([back, below], axis=1)
            pick = scatter[:, band:, :, band:].reshape(slices * band, angles * 2 * band)
            before = current[:, band:]
        else:
            window = jnp.concatenate([lax.ppermute(back, SLAB, down_ring), back, below], axis=1)
            pick = scatter.reshape(slices * 2 * band, angles * 3 * band)
            before = current
        gradient = jnp.dot(pick, window.reshape(-1, chunk), preferred_element_type=f32)
        current = (before.astype(f32) - STEP_SIZE * gradient.reshape(before.shape)).astype(bf16)

    lanes = 128
    dots = jnp.stack(split_parts(jnp.sum(projection * slope_field, axis=(1, 2)), 3))
    dots = jnp.pad(dots.reshape(1, -1), ((0, band - 1), (0, lanes - dots.size)))
    dots = jnp.broadcast_to(dots, (slabs, 1, band, lanes))
    home = current.reshape(slabs, slices_here, band, chunk // lanes, lanes).transpose(0, 1, 3, 2, 4)
    home = home.reshape(slabs, -1, band, lanes)
    home = lax.all_to_all(jnp.concatenate([home, dots], axis=1), SLAB, 0, 0, tiled=True)
    dots = home[:, -1, 0, : 3 * angles_here].astype(f32).reshape(slabs, 3, angles_here)
    shift_slope = jnp.sum(dots, axis=(0, 1)) / math.sqrt(rows_all * columns)
    home = home[:, :-1].reshape(slabs, slices_here, chunk // lanes, band, lanes)
    home = home.transpose(1, 0, 3, 2, 4).reshape(slices_here, rows_all, chunk)
    ahead = [(i, (i + 1) % angs) for i in range(angs)]
    behind = [((i + 1) % angs, i) for i in range(angs)]
    half = slices_here // 2
    lower = lax.ppermute(home, "ang", ahead)
    upper = lax.ppermute(home, "ang", behind)
    far = [lax.ppermute(lower[:half], "ang", ahead), lax.ppermute(upper[half:], "ang", behind)]
    updated = in_order([home, upper, jnp.concatenate(far), lower])
    return updated, residual, shift_slope


def solution(mesh):
    return jax.shard_map(
        per_device,
        mesh=mesh,
        in_specs=(
            P(("grp", SLAB), None, None),
            P("ang", None, None),
            P("ang", None),
            P(("grp", "ang"), SLAB, None),
            P(("grp", "ang")),
        ),
        out_specs=(P(("grp", SLAB), None, None), P(("grp", "ang"), SLAB, None), P(("grp", "ang"))),
        check_vma=False,
    )
```

```python
import math

import jax
import jax.numpy as jnp
from jax import lax
from jax.sharding import PartitionSpec as P


ROUNDS = 2
STEP_SIZE = 0.5


def moments(length):
    waves = [2.0 * math.pi * k / length for k in range(-(length // 2), length // 2)]
    return [sum(w**p for w in waves) / length for p in (2, 4, 6, 8)]


def interpolation_kernels(shifts, taps, length):
    whole = jnp.round(shifts)
    part = shifts - whole
    odd_shift = 1.0 - 2.0 * (whole.astype(jnp.int32) & 1).astype(jnp.float32)
    sine = odd_shift * jnp.sin(math.pi * part)
    cosine = odd_shift * jnp.cos(math.pi * part)
    v = lax.broadcasted_iota(jnp.int32, (1, taps, length), 1)
    u = lax.broadcasted_iota(jnp.int32, (1, taps, length), 2)
    lag = u - v
    lag = jnp.where(lag >= length // 2, lag - length, jnp.where(lag < -(length // 2), lag + length, lag))
    sign = 1.0 - 2.0 * (lag & 1).astype(jnp.float32)
    d = (lag - whole.astype(jnp.int32)[:, None, None]).astype(jnp.float32) - part[:, None, None]
    near = jnp.abs(d) < 0.1
    safe = jnp.where(near, 1.0, d)
    y = safe * (math.pi / length)
    sin_y = jnp.sin(y)
    cos_y = jnp.cos(y)
    inv = 1.0 / sin_y
    cot = cos_y * inv
    sin_d = -sign * sine[:, None, None]
    cos_d = sign * cosine[:, None, None]
    far_h = sin_d * cot * (1.0 / length)
    far_q = (math.pi / length) * (sin_d * inv * inv * (1.0 / length) - cos_d * cot)
    m2, m4, m6, m8 = moments(length)
    s = d * d
    near_h = 1.0 - s * (m2 / 2 - s * (m4 / 24 - s * (m6 / 720 - s * (m8 / 40320))))
    near_q = d * (m2 - s * (m4 / 6 - s * (m6 / 120 - s * (m8 / 5040))))
    return jnp.where(near, near_h, far_h), jnp.where(near, near_q, far_q)


def registered(measured, shifts):
    angles, rows, length = measured.shape
    taps = 128
    blocks = length // taps
    h, q = interpolation_kernels(shifts, taps, length)
    kernels = jnp.concatenate([h, q], axis=2)
    pieces = measured.reshape(angles, rows, blocks, taps).transpose(0, 2, 1, 3)
    pieces = pieces.reshape(angles, blocks * rows, taps)
    spread = jnp.einsum("avr,aru->avu", pieces, kernels, precision=lax.Precision.HIGHEST)
    spread = spread.reshape(angles, blocks, rows, 2, length)
    total = spread[:, 0]
    for k in range(1, blocks):
        total = total + jnp.roll(spread[:, k], taps * k, axis=-1)
    return total[:, :, 0], total[:, :, 1]


SLAB = "slab"


def from_ang(blocks, step):
    size = len(blocks)
    return [
        blocks[k] if k == 0 else lax.ppermute(blocks[k], "ang", [(i, (i + k * step) % size) for i in range(size)])
        for k in range(size)
    ]


def split_parts(value, count):
    parts = []
    for _ in range(count):
        high = lax.reduce_precision(value, 8, 7)
        parts.append(high.astype(jnp.bfloat16))
        value = value - high
    return parts


def in_order(chunks):
    count = len(chunks)
    here = lax.axis_index("ang")

    def pick(column):
        found = chunks[column]
        for k in range(1, count):
            found = jnp.where(here == k, chunks[(column - k) % count], found)
        return found

    return jnp.concatenate([pick(column) for column in range(count)], axis=2)


def per_device(volume, ray_weights, row_offsets, measured, shifts):
    slices_here, rows_all, cells = volume.shape
    angles_here, band, columns = measured.shape
    slabs = lax.axis_size(SLAB)
    angs = lax.axis_size("ang")
    here = lax.axis_index("ang")
    chunk = cells // angs
    slices = slices_here * slabs
    angles = angles_here * angs
    f32 = jnp.float32
    bf16 = jnp.bfloat16
    down_ring = [(i, i + 1) for i in range(slabs - 1)]
    up_ring = [(i + 1, i) for i in range(slabs - 1)]

    table = from_ang([row_offsets] * angs, -1)
    table = jnp.stack(table).reshape(angles, slices)

    mine = lax.dynamic_slice_in_dim(volume, here * chunk, chunk, 2)
    mine = mine.reshape(slices_here, slabs, band, chunk).transpose(1, 0, 2, 3)
    own = lax.all_to_all(mine, SLAB, 0, 0, tiled=True)
    own = own.reshape(slices, band, chunk)
    above = lax.ppermute(own, SLAB, down_ring)
    current = jnp.concatenate([above, own], axis=1)

    weights = [
        lax.dynamic_slice_in_dim(ray_weights, (here + angs - k) % angs * chunk, chunk, 1) for k in range(angs)
    ]

    shifted, slope_field = registered(measured, shifts)

    places = slices * 2 * band
    spread = lax.broadcasted_iota(jnp.int32, (slices, places), 0) == lax.broadcasted_iota(
        jnp.int32, (slices, places), 1
    ) // (2 * band)
    offsets = jnp.dot(table.astype(bf16), spread.astype(bf16), preferred_element_type=f32)
    shape = (angles, band, places)
    y = lax.broadcasted_iota(jnp.int32, shape, 1)
    r = lax.broadcasted_iota(jnp.int32, shape, 2) % (2 * band)
    held = (r >= band) | (lax.axis_index(SLAB) > 0)
    gather = (y - (r - band) == offsets.astype(jnp.int32)[:, None, :]) & held
    gather = gather.astype(bf16).reshape(angles * band, places)
    shape = (slices, 2 * band, angles, 3 * band)
    r = lax.broadcasted_iota(jnp.int32, shape, 1)
    t = lax.broadcasted_iota(jnp.int32, shape, 3)
    scatter = (t == r + table.T[:, None, :, None]).astype(bf16)

    for round_index in range(ROUNDS):
        last = round_index == ROUNDS - 1
        stacked = jnp.dot(gather, current.reshape(slices * 2 * band, chunk), preferred_element_type=f32)
        high, low = (
            x.reshape(angs, angles_here, band, chunk) for x in split_parts(stacked, 2)
        )
        parts = from_ang([jnp.concatenate([high[k], low[k]], axis=1) for k in range(angs)], 1)
        product = sum(
            jnp.einsum("arx,axu->aru", x, w, preferred_element_type=f32) for x, w in zip(parts, weights)
        )
        projection = product[:, :band] + product[:, band:]
        residual = projection - shifted
        rounded = residual.astype(bf16)
        back = [
            jnp.einsum("aru,axu->arx", rounded, w, preferred_element_type=f32).astype(bf16) for w in weights
        ]
        back = from_ang(back, -1)
        back = jnp.concatenate(back, axis=0)
        below = lax.ppermute(back, SLAB, up_ring)
        if last:
            window = jnp.concatenate([back, below], axis=1)
            pick = scatter[:, band:, :, band:].reshape(slices * band, angles * 2 * band)
            before = current[:, band:]
        else:
            window = jnp.concatenate([lax.ppermute(back, SLAB, down_ring), back, below], axis=1)
            pick = scatter.reshape(slices * 2 * band, angles * 3 * band)
            before = current
        gradient = jnp.dot(pick, window.reshape(-1, chunk), preferred_element_type=f32)
        current = (before.astype(f32) - STEP_SIZE * gradient.reshape(before.shape)).astype(bf16)

    home = current.reshape(slabs, slices_here, band, chunk)
    home = lax.all_to_all(home, SLAB, 0, 0, tiled=True)
    home = home.transpose(1, 0, 2, 3).reshape(slices_here, rows_all, chunk)
    dots = jnp.sum(projection * slope_field, axis=(1, 2))
    bit = 1
    while bit < slabs:
        dots = dots + lax.ppermute(dots, SLAB, [(i, i ^ bit) for i in range(slabs)])
        bit *= 2
    shift_slope = dots * (1.0 / math.sqrt(rows_all * columns))
    ahead = [(i, (i + 1) % angs) for i in range(angs)]
    behind = [((i + 1) % angs, i) for i in range(angs)]
    half = slices_here // 2
    lower = lax.ppermute(home, "ang", ahead)
    upper = lax.ppermute(home, "ang", behind)
    far = [lax.ppermute(lower[:half], "ang", ahead), lax.ppermute(upper[half:], "ang", behind)]
    updated = in_order([home, upper, jnp.concatenate(far), lower])
    return updated, residual, shift_slope


def solution(mesh):
    return jax.shard_map(
        per_device,
        mesh=mesh,
        in_specs=(
            P(("grp", SLAB), None, None),
            P("ang", None, None),
            P("ang", None),
            P(("grp", "ang"), SLAB, None),
            P(("grp", "ang")),
        ),
        out_specs=(P(("grp", SLAB), None, None), P(("grp", "ang"), SLAB, None), P(("grp", "ang"))),
        check_vma=False,
    )
```

```python
import math

import jax
import jax.numpy as jnp
from jax import lax
from jax.sharding import PartitionSpec as P


ROUNDS = 2
STEP_SIZE = 0.5


def moments(length):
    waves = [2.0 * math.pi * k / length for k in range(-(length // 2), length // 2)]
    return [sum(w**p for w in waves) / length for p in range(2, 16, 2)]


def series(square, terms):
    total = terms[-1]
    for term in terms[-2::-1]:
        total = term - square * total
    return total


def interpolation_kernels(shifts, taps, length):
    whole = jnp.round(shifts)
    part = (shifts - whole)[:, None, None]
    whole = whole.astype(jnp.int32)[:, None, None]
    odd_shift = 1.0 - 2.0 * (whole & 1).astype(jnp.float32)
    sine = odd_shift * jnp.sin(math.pi * part)
    cosine = odd_shift * jnp.cos(math.pi * part)
    step = math.pi / length
    v = lax.broadcasted_iota(jnp.int32, (1, taps, 1), 1) - taps // 2
    u = lax.broadcasted_iota(jnp.int32, (1, 1, length), 2) - taps // 2
    u = jnp.where(u >= length // 2, u - length, u)
    sign = (1.0 - 2.0 * (v & 1).astype(jnp.float32)) * (1.0 - 2.0 * (u & 1).astype(jnp.float32))
    ahead = ((u - whole).astype(jnp.float32) - part) * step
    behind = v.astype(jnp.float32) * step
    sin_u, cos_u, sin_v, cos_v = jnp.sin(ahead), jnp.cos(ahead), jnp.sin(behind), jnp.cos(behind)
    sin_y = sin_u * cos_v - cos_u * sin_v
    cos_y = cos_u * cos_v + sin_u * sin_v
    d = (u - v - whole).astype(jnp.float32) - part
    near = jnp.abs(d) <= 0.5
    inv = 1.0 / jnp.where(near, 1.0, sin_y)
    cot = cos_y * inv
    sin_d = -sign * sine
    far_h = sin_d * cot * (1.0 / length)
    far_q = step * (sin_d * (inv * inv) * (1.0 / length) - sign * cosine * cot)
    rates = moments(length)
    near_h = series(d * d, [1.0] + [m / math.factorial(2 * k + 2) for k, m in enumerate(rates)])
    near_q = d * series(d * d, [m / math.factorial(2 * k + 1) for k, m in enumerate(rates)])
    return jnp.where(near, near_h, far_h), jnp.where(near, near_q, far_q)


def registered(measured, shifts):
    angles, rows, length = measured.shape
    taps = 128
    blocks = length // taps
    h, q = interpolation_kernels(shifts, taps, length)
    kernels = jnp.concatenate([h, q], axis=2)
    pieces = measured.reshape(angles, rows, blocks, taps).transpose(0, 2, 1, 3)
    pieces = pieces.reshape(angles, blocks * rows, taps)
    spread = jnp.einsum("avr,aru->avu", pieces, kernels, precision=lax.Precision.HIGHEST)
    spread = spread.reshape(angles, blocks, rows, 2, length)
    total = spread[:, 0]
    for k in range(1, blocks):
        total = total + jnp.roll(spread[:, k], taps * k, axis=-1)
    return total[:, :, 0], total[:, :, 1]


SLAB = "slab"


def from_ang(blocks, step):
    size = len(blocks)
    return [
        blocks[k] if k == 0 else lax.ppermute(blocks[k], "ang", [(i, (i + k * step) % size) for i in range(size)])
        for k in range(size)
    ]


def split_parts(value, count):
    parts = []
    for _ in range(count):
        high = lax.reduce_precision(value, 8, 7)
        parts.append(high.astype(jnp.bfloat16))
        value = value - high
    return parts


def in_order(chunks):
    count = len(chunks)
    here = lax.axis_index("ang")

    def pick(column):
        found = chunks[column]
        for k in range(1, count):
            found = jnp.where(here == k, chunks[(column - k) % count], found)
        return found

    return jnp.concatenate([pick(column) for column in range(count)], axis=2)


def per_device(volume, ray_weights, row_offsets, measured, shifts):
    slices_here, rows_all, cells = volume.shape
    angles_here, band, columns = measured.shape
    slabs = lax.axis_size(SLAB)
    angs = lax.axis_size("ang")
    here = lax.axis_index("ang")
    chunk = cells // angs
    slices = slices_here * slabs
    angles = angles_here * angs
    f32 = jnp.float32
    bf16 = jnp.bfloat16
    down_ring = [(i, i + 1) for i in range(slabs - 1)]
    up_ring = [(i + 1, i) for i in range(slabs - 1)]

    table = from_ang([row_offsets] * angs, -1)
    table = jnp.stack(table).reshape(angles, slices)

    mine = lax.dynamic_slice_in_dim(volume, here * chunk, chunk, 2)
    mine = mine.reshape(slices_here, slabs, band, chunk).transpose(1, 0, 2, 3)
    own = lax.all_to_all(mine, SLAB, 0, 0, tiled=True)
    own = own.reshape(slices, band, chunk)
    above = lax.ppermute(own, SLAB, down_ring)
    current = jnp.concatenate([above, own], axis=1)

    weights = [
        lax.dynamic_slice_in_dim(ray_weights, (here + angs - k) % angs * chunk, chunk, 1) for k in range(angs)
    ]

    shifted, slope_field = registered(measured, shifts)

    places = slices * 2 * band
    spread = lax.broadcasted_iota(jnp.int32, (slices, places), 0) == lax.broadcasted_iota(
        jnp.int32, (slices, places), 1
    ) // (2 * band)
    offsets = jnp.dot(table.astype(bf16), spread.astype(bf16), preferred_element_type=f32)
    shape = (angles, band, places)
    y = lax.broadcasted_iota(jnp.int32, shape, 1)
    r = lax.broadcasted_iota(jnp.int32, shape, 2) % (2 * band)
    held = (r >= band) | (lax.axis_index(SLAB) > 0)
    gather = (y - (r - band) == offsets.astype(jnp.int32)[:, None, :]) & held
    gather = gather.astype(bf16).reshape(angles * band, places)
    shape = (slices, 2 * band, angles, 3 * band)
    r = lax.broadcasted_iota(jnp.int32, shape, 1)
    t = lax.broadcasted_iota(jnp.int32, shape, 3)
    scatter = (t == r + table.T[:, None, :, None]).astype(bf16)

    for round_index in range(ROUNDS):
        last = round_index == ROUNDS - 1
        stacked = jnp.dot(gather, current.reshape(slices * 2 * band, chunk), preferred_element_type=f32)
        high, low = (
            x.reshape(angs, angles_here, band, chunk) for x in split_parts(stacked, 2)
        )
        parts = from_ang([jnp.concatenate([high[k], low[k]], axis=1) for k in range(angs)], 1)
        product = sum(
            jnp.einsum("arx,axu->aru", x, w, preferred_element_type=f32) for x, w in zip(parts, weights)
        )
        projection = product[:, :band] + product[:, band:]
        residual = projection - shifted
        rounded = residual.astype(bf16)
        back = [
            jnp.einsum("aru,axu->arx", rounded, w, preferred_element_type=f32).astype(bf16) for w in weights
        ]
        back = from_ang(back, -1)
        back = jnp.concatenate(back, axis=0)
        below = lax.ppermute(back, SLAB, up_ring)
        if last:
            window = jnp.concatenate([back, below], axis=1)
            pick = scatter[:, band:, :, band:].reshape(slices * band, angles * 2 * band)
            before = current[:, band:]
        else:
            window = jnp.concatenate([lax.ppermute(back, SLAB, down_ring), back, below], axis=1)
            pick = scatter.reshape(slices * 2 * band, angles * 3 * band)
            before = current
        gradient = jnp.dot(pick, window.reshape(-1, chunk), preferred_element_type=f32)
        current = (before.astype(f32) - STEP_SIZE * gradient.reshape(before.shape)).astype(bf16)

    home = current.reshape(slabs, slices_here, band, chunk)
    home = lax.all_to_all(home, SLAB, 0, 0, tiled=True)
    home = home.transpose(1, 0, 2, 3).reshape(slices_here, rows_all, chunk)
    dots = jnp.broadcast_to(jnp.sum(projection * slope_field, axis=(1, 2)), (slabs, angles_here))
    dots = lax.all_to_all(dots, SLAB, 0, 0, tiled=True)
    dots = jnp.sum(dots, axis=0)
    shift_slope = dots * (1.0 / math.sqrt(rows_all * columns))
    ahead = [(i, (i + 1) % angs) for i in range(angs)]
    behind = [((i + 1) % angs, i) for i in range(angs)]
    half = slices_here // 2
    lower = lax.ppermute(home, "ang", ahead)
    upper = lax.ppermute(home, "ang", behind)
    far = [lax.ppermute(lower[:half], "ang", ahead), lax.ppermute(upper[half:], "ang", behind)]
    updated = in_order([home, upper, jnp.concatenate(far), lower])
    return updated, residual, shift_slope


def solution(mesh):
    return jax.shard_map(
        per_device,
        mesh=mesh,
        in_specs=(
            P(("grp", SLAB), None, None),
            P("ang", None, None),
            P("ang", None),
            P(("grp", "ang"), SLAB, None),
            P(("grp", "ang")),
        ),
        out_specs=(P(("grp", SLAB), None, None), P(("grp", "ang"), SLAB, None), P(("grp", "ang"))),
        check_vma=False,
    )
```

```python
import math

import jax
import jax.numpy as jnp
from jax import lax
from jax.sharding import PartitionSpec as P


ROUNDS = 2
STEP_SIZE = 0.5


def moments(length):
    waves = [2.0 * math.pi * k / length for k in range(-(length // 2), length // 2)]
    return [sum(w**p for w in waves) / length for p in range(2, 16, 2)]


def series(square, terms):
    total = terms[-1]
    for term in terms[-2::-1]:
        total = term - square * total
    return total


def interpolation_kernels(shifts, taps, length):
    whole = jnp.round(shifts)
    part = (shifts - whole)[:, None, None]
    whole = whole.astype(jnp.int32)[:, None, None]
    odd_shift = 1.0 - 2.0 * (whole & 1).astype(jnp.float32)
    sine = odd_shift * jnp.sin(math.pi * part)
    cosine = odd_shift * jnp.cos(math.pi * part)
    step = math.pi / length
    v = lax.broadcasted_iota(jnp.int32, (1, taps, 1), 1) - taps // 2
    u = lax.broadcasted_iota(jnp.int32, (1, 1, length), 2) - taps // 2
    u = jnp.where(u >= length // 2, u - length, u)
    sign = (1.0 - 2.0 * (v & 1).astype(jnp.float32)) * (1.0 - 2.0 * (u & 1).astype(jnp.float32))
    ahead = ((u - whole).astype(jnp.float32) - part) * step
    behind = v.astype(jnp.float32) * step
    sin_u, cos_u, sin_v, cos_v = jnp.sin(ahead), jnp.cos(ahead), jnp.sin(behind), jnp.cos(behind)
    sin_y = sin_u * cos_v - cos_u * sin_v
    cos_y = cos_u * cos_v + sin_u * sin_v
    d = (u - v - whole).astype(jnp.float32) - part
    near = jnp.abs(d) <= 0.5
    inv = 1.0 / jnp.where(near, 1.0, sin_y)
    cot = cos_y * inv
    sin_d = -sign * sine
    far_h = sin_d * cot * (1.0 / length)
    far_q = step * (sin_d * (inv * inv) * (1.0 / length) - sign * cosine * cot)
    rates = moments(length)
    near_h = series(d * d, [1.0] + [m / math.factorial(2 * k + 2) for k, m in enumerate(rates)])
    near_q = d * series(d * d, [m / math.factorial(2 * k + 1) for k, m in enumerate(rates)])
    return jnp.where(near, near_h, far_h), jnp.where(near, near_q, far_q)


def registered(measured, shifts):
    angles, rows, length = measured.shape
    taps = 128
    blocks = length // taps
    h, q = interpolation_kernels(shifts, taps, length)
    kernels = jnp.concatenate([h, q], axis=2)
    pieces = measured.reshape(angles, rows, blocks, taps).transpose(0, 2, 1, 3)
    pieces = pieces.reshape(angles, blocks * rows, taps)
    spread = jnp.einsum("avr,aru->avu", pieces, kernels, precision=lax.Precision.HIGHEST)
    spread = spread.reshape(angles, blocks, rows, 2, length)
    total = spread[:, 0]
    for k in range(1, blocks):
        total = total + jnp.roll(spread[:, k], taps * k, axis=-1)
    return total[:, :, 0], total[:, :, 1]


SLAB = "slab"


def from_ang(blocks, step):
    size = len(blocks)
    return [
        blocks[k] if k == 0 else lax.ppermute(blocks[k], "ang", [(i, (i + k * step) % size) for i in range(size)])
        for k in range(size)
    ]


def split_parts(value, count):
    parts = []
    for _ in range(count):
        high = lax.reduce_precision(value, 8, 7)
        parts.append(high.astype(jnp.bfloat16))
        value = value - high
    return parts


def in_order(chunks):
    count = len(chunks)
    here = lax.axis_index("ang")

    def pick(column):
        found = chunks[column]
        for k in range(1, count):
            found = jnp.where(here == k, chunks[(column - k) % count], found)
        return found

    return jnp.concatenate([pick(column) for column in range(count)], axis=2)


def per_device(volume, ray_weights, row_offsets, measured, shifts):
    slices_here, rows_all, cells = volume.shape
    angles_here, band, columns = measured.shape
    slabs = lax.axis_size(SLAB)
    angs = lax.axis_size("ang")
    here = lax.axis_index("ang")
    chunk = cells // angs
    slices = slices_here * slabs
    angles = angles_here * angs
    f32 = jnp.float32
    bf16 = jnp.bfloat16
    down_ring = [(i, i + 1) for i in range(slabs - 1)]
    up_ring = [(i + 1, i) for i in range(slabs - 1)]

    table = from_ang([row_offsets] * angs, -1)
    table = jnp.stack(table).reshape(angles, slices)

    mine = lax.dynamic_slice_in_dim(volume, here * chunk, chunk, 2)
    mine = mine.reshape(slices_here, slabs, band, chunk).transpose(1, 0, 2, 3)
    own = lax.all_to_all(mine, SLAB, 0, 0, tiled=True)
    own = own.reshape(slices, band, chunk)
    above = lax.ppermute(own, SLAB, down_ring)
    current = jnp.concatenate([above, own], axis=1)

    weights = [
        lax.dynamic_slice_in_dim(ray_weights, (here + angs - k) % angs * chunk, chunk, 1) for k in range(angs)
    ]

    shifted, slope_field = registered(measured, shifts)

    places = slices * 2 * band
    spread = lax.broadcasted_iota(jnp.int32, (slices, places), 0) == lax.broadcasted_iota(
        jnp.int32, (slices, places), 1
    ) // (2 * band)
    offsets = jnp.dot(table.astype(bf16), spread.astype(bf16), preferred_element_type=f32)
    shape = (angles, band, places)
    y = lax.broadcasted_iota(jnp.int32, shape, 1)
    r = lax.broadcasted_iota(jnp.int32, shape, 2) % (2 * band)
    held = (r >= band) | (lax.axis_index(SLAB) > 0)
    gather = (y - (r - band) == offsets.astype(jnp.int32)[:, None, :]) & held
    gather = gather.astype(bf16).reshape(angles * band, places)
    shape = (slices, 2 * band, angles, 3 * band)
    r = lax.broadcasted_iota(jnp.int32, shape, 1)
    t = lax.broadcasted_iota(jnp.int32, shape, 3)
    scatter = (t == r + table.T[:, None, :, None]).astype(bf16)

    for round_index in range(ROUNDS):
        last = round_index == ROUNDS - 1
        stacked = jnp.dot(gather, current.reshape(slices * 2 * band, chunk), preferred_element_type=f32)
        high, low = (
            x.reshape(angs, angles_here, band, chunk) for x in split_parts(stacked, 2)
        )
        parts = from_ang([jnp.concatenate([high[k], low[k]], axis=1) for k in range(angs)], 1)
        product = sum(
            jnp.einsum("arx,axu->aru", x, w, preferred_element_type=f32) for x, w in zip(parts, weights)
        )
        projection = product[:, :band] + product[:, band:]
        residual = projection - shifted
        rounded = residual.astype(bf16)
        back = [
            jnp.einsum("aru,axu->arx", rounded, w, preferred_element_type=f32).astype(bf16) for w in weights
        ]
        back = from_ang(back, -1)
        back = jnp.concatenate(back, axis=0)
        below = lax.ppermute(back, SLAB, up_ring)
        if last:
            window = jnp.concatenate([back, below], axis=1)
            pick = scatter[:, band:, :, band:].reshape(slices * band, angles * 2 * band)
            before = current[:, band:]
        else:
            window = jnp.concatenate([lax.ppermute(back, SLAB, down_ring), back, below], axis=1)
            pick = scatter.reshape(slices * 2 * band, angles * 3 * band)
            before = current
        gradient = jnp.dot(pick, window.reshape(-1, chunk), preferred_element_type=f32)
        current = (before.astype(f32) - STEP_SIZE * gradient.reshape(before.shape)).astype(bf16)

    lanes = 128
    dots = jnp.stack(split_parts(jnp.sum(projection * slope_field, axis=(1, 2)), 3))
    dots = jnp.pad(dots.reshape(1, -1), ((0, band - 1), (0, lanes - dots.size)))
    dots = jnp.broadcast_to(dots, (slabs, 1, band, lanes))
    home = current.reshape(slabs, slices_here, band, chunk // lanes, lanes).transpose(0, 1, 3, 2, 4)
    home = home.reshape(slabs, -1, band, lanes)
    home = lax.all_to_all(jnp.concatenate([home, dots], axis=1), SLAB, 0, 0, tiled=True)
    dots = home[:, -1, 0, : 3 * angles_here].astype(f32).reshape(slabs, 3, angles_here)
    shift_slope = jnp.sum(dots, axis=(0, 1)) / math.sqrt(rows_all * columns)
    home = home[:, :-1].reshape(slabs, slices_here, chunk // lanes, band, lanes)
    home = home.transpose(1, 0, 3, 2, 4).reshape(slices_here, rows_all, chunk)
    ahead = [(i, (i + 1) % angs) for i in range(angs)]
    behind = [((i + 1) % angs, i) for i in range(angs)]
    half = slices_here // 2
    lower = lax.ppermute(home, "ang", ahead)
    upper = lax.ppermute(home, "ang", behind)
    far = [lax.ppermute(lower[:half], "ang", ahead), lax.ppermute(upper[half:], "ang", behind)]
    updated = in_order([home, upper, jnp.concatenate(far), lower])
    return updated, residual, shift_slope


def solution(mesh):
    return jax.shard_map(
        per_device,
        mesh=mesh,
        in_specs=(
            P(("grp", SLAB), None, None),
            P("ang", None, None),
            P("ang", None),
            P(("grp", "ang"), SLAB, None),
            P(("grp", "ang")),
        ),
        out_specs=(P(("grp", SLAB), None, None), P(("grp", "ang"), SLAB, None), P(("grp", "ang"))),
        check_vma=False,
    )
```
